32 devices in a mesh: dp: 8 (over z, y), fsdp: 4 (over x, core).
Axes of the slice: x: 2, y: 2, z: 4, core: 2. Of those that a mesh axis runs over, the one named last changes fastest.
Arguments:
- tokens: int32 [96, 512], P(('dp', 'fsdp'))
- grad_y: bfloat16 [96, 512, 1280], P(('dp', 'fsdp'))
- embedding: bfloat16 [33, 1280], P(None, 'fsdp')
- ln1_gain: bfloat16 [1280], P('fsdp')
- ln1_bias: bfloat16 [1280], P('fsdp')
- w_qkv: bfloat16 [1280, 3840], P('fsdp')
- b_qkv: bfloat16 [3840], P('fsdp')
- w_out: bfloat16 [1280, 1280], P('fsdp')
- b_out: bfloat16 [1280], P('fsdp')
- ln2_gain: bfloat16 [1280], P('fsdp')
- ln2_bias: bfloat16 [1280], P('fsdp')
- w_fc1: bfloat16 [1280, 5120], P('fsdp')
- b_fc1: bfloat16 [5120], P('fsdp')
- w_fc2: bfloat16 [5120, 1280], P('fsdp')
- b_fc2: bfloat16 [1280], P('fsdp')
Outputs:
- output 1: bfloat16 [96, 512, 1280], P(('dp', 'fsdp'))
- output 2: float32 [33, 1280], P(None, 'fsdp')
- output 3: float32 [1280], P('fsdp')
- output 4: float32 [1280], P('fsdp')
- output 5: float32 [1280, 3840], P('fsdp')
- output 6: float32 [3840], P('fsdp')
- output 7: float32 [1280, 1280], P('fsdp')
- output 8: float32 [1280], P('fsdp')
- output 9: float32 [1280], P('fsdp')
- output 10: float32 [1280], P('fsdp')
- output 11: float32 [1280, 5120], P('fsdp')
- output 12: float32 [5120], P('fsdp')
- output 13: float32 [5120, 1280], P('fsdp')
- output 14: float32 [1280], P('fsdp')
All inputs are finite; a program needn't handle non-finite values.
Results may differ from the reference program's by a relative error of at most 0.0115641.
Values are sent between devices in bfloat16 or wider.
A program may use at most 1 GiB of HBM per device.

```python
import jax
import jax.numpy as jnp
from jax import lax

D = 1280
HEADS = 20
FF = 5120
SEQ = 512
BATCH = 96
VOCAB = 33
CLS_ID = 0
PAD_ID = 1
EOS_ID = 2
MASK_ID = 32

HEAD_DIM = D // HEADS
MASK_RATIO = 0.15 * 0.8
LN_EPS = 1e-5
ROPE_BASE = 10000.0


def draw_tokens(tok_key):
    len_key, res_key, rate_key, pick_key = jax.random.split(tok_key, 4)
    lengths = jax.random.randint(len_key, (BATCH,), SEQ // 2, SEQ + 1)
    lengths = lengths.at[0].set(SEQ).at[1].set(SEQ // 2)
    position = jnp.arange(SEQ)[None, :]
    residues = jax.random.randint(res_key, (BATCH, SEQ), 4, 29)
    mask_rate = jax.random.randint(rate_key, (BATCH, 1), 5, 26)
    pick_draw = jax.random.randint(pick_key, (BATCH, SEQ), 0, 100)
    body_tok = jnp.where(pick_draw < mask_rate, MASK_ID, residues)
    last_pos = lengths[:, None] - 1
    tok_grid = jnp.where(position < last_pos, body_tok, PAD_ID)
    tok_grid = jnp.where(position == last_pos, EOS_ID, tok_grid)
    return jnp.where(position == 0, CLS_ID, tok_grid).astype(jnp.int32)


def setup_inputs(seed: int = 0) -> dict:
    keys = jax.random.split(jax.random.key(seed), 16)

    def draw_normal(sub_key, dims, std_scale, offset=0.0):
        return (jax.random.normal(sub_key, dims, jnp.float32) * std_scale + offset).astype(jnp.bfloat16)

    return {
        'tokens': draw_tokens(keys[0]),
        'grad_y': draw_normal(keys[1], (BATCH, SEQ, D), 1.0),
        'embedding': draw_normal(keys[2], (VOCAB, D), 1.0),
        'ln1_gain': draw_normal(keys[3], (D,), 0.2, 1.0),
        'ln1_bias': draw_normal(keys[4], (D,), 0.2),
        'w_qkv': draw_normal(keys[5], (D, 3 * D), D ** -0.5),
        'b_qkv': draw_normal(keys[6], (3 * D,), 0.2),
        'w_out': draw_normal(keys[7], (D, D), D ** -0.5),
        'b_out': draw_normal(keys[8], (D,), 0.2),
        'ln2_gain': draw_normal(keys[9], (D,), 0.2, 1.0),
        'ln2_bias': draw_normal(keys[10], (D,), 0.2),
        'w_fc1': draw_normal(keys[11], (D, FF), D ** -0.5),
        'b_fc1': draw_normal(keys[12], (FF,), 0.2),
        'w_fc2': draw_normal(keys[13], (FF, D), FF ** -0.5),
        'b_fc2': draw_normal(keys[14], (D,), 0.2),
    }


def to_bf16(x_val):
    return x_val.astype(jnp.bfloat16).astype(jnp.float32)


def mat_mul(lhs, rhs):
    return jnp.dot(lhs, rhs, preferred_element_type=jnp.float32)


def layer_norm(x_val, gain, bias):
    centered = x_val - jnp.mean(x_val, axis=-1, keepdims=True)
    row_var = jnp.mean(centered * centered, axis=-1, keepdims=True)
    return centered * lax.rsqrt(row_var + LN_EPS) * gain + bias


def rope_tables():
    inv_freq = 1.0 / (ROPE_BASE ** (jnp.arange(0, HEAD_DIM, 2, dtype=jnp.float32) / HEAD_DIM))
    angles = jnp.arange(SEQ, dtype=jnp.float32)[:, None] * inv_freq[None, :]
    return jnp.cos(angles)[:, None, :], jnp.sin(angles)[:, None, :]


def rotate(x_val, cos_tab, sin_tab):
    half_dim = x_val.shape[-1] // 2
    low_half = x_val[..., :half_dim]
    high_half = x_val[..., half_dim:]
    return jnp.concatenate([low_half * cos_tab - high_half * sin_tab, high_half * cos_tab + low_half * sin_tab], axis=-1)


def seq_forward(weights, tok_row):
    (embedding, ln1_gain, ln1_bias, w_qkv, b_qkv, w_out, b_out,
     ln2_gain, ln2_bias, w_fc1, b_fc1, w_fc2, b_fc2) = weights
    is_mask = tok_row == MASK_ID
    is_pad = tok_row == PAD_ID
    mask_count = jnp.sum(is_mask.astype(jnp.float32))
    real_count = jnp.sum(jnp.logical_not(is_pad).astype(jnp.float32))
    factor = (1.0 - MASK_RATIO) / (1.0 - mask_count / real_count)
    keep_scale = jnp.where(is_mask | is_pad, 0.0, factor)
    x_in = to_bf16(embedding[tok_row] * keep_scale[:, None])
    h_one = to_bf16(layer_norm(x_in, ln1_gain, ln1_bias))
    qkv_proj = (mat_mul(h_one, w_qkv) + b_qkv).reshape(SEQ, 3, HEADS, HEAD_DIM)
    cos_tab, sin_tab = rope_tables()
    queries = to_bf16(rotate(qkv_proj[:, 0] * HEAD_DIM ** -0.5, cos_tab, sin_tab))
    key_rows = to_bf16(rotate(qkv_proj[:, 1], cos_tab, sin_tab))
    values = to_bf16(qkv_proj[:, 2])
    scores = jnp.einsum('qhd,khd->hqk', queries, key_rows)
    scores = jnp.where(is_pad[None, None, :], -1e30, scores)
    attn_prob = to_bf16(jax.nn.softmax(scores, axis=-1))
    context = to_bf16(jnp.einsum('hqk,khd->qhd', attn_prob, values)).reshape(SEQ, D)
    x_mid = x_in + mat_mul(context, w_out) + b_out
    h_two = to_bf16(layer_norm(x_mid, ln2_gain, ln2_bias))
    hidden_act = to_bf16(jax.nn.gelu(mat_mul(h_two, w_fc1) + b_fc1, approximate=False))
    return to_bf16(x_mid + mat_mul(hidden_act, w_fc2) + b_fc2)


def reference(tokens, grad_y, embedding, ln1_gain, ln1_bias, w_qkv, b_qkv, w_out, b_out,
              ln2_gain, ln2_bias, w_fc1, b_fc1, w_fc2, b_fc2):
    weights = tuple(w.astype(jnp.float32) for w in (embedding, ln1_gain, ln1_bias, w_qkv, b_qkv, w_out, b_out,
                                                     ln2_gain, ln2_bias, w_fc1, b_fc1, w_fc2, b_fc2))
    grad_init = tuple(jnp.zeros_like(w) for w in weights)

    def scan_step(grad_sum, seq_pair):
        tok_row, dy_row = seq_pair
        y_row, pull_back = jax.vjp(lambda params: seq_forward(params, tok_row), weights)
        grad_row = pull_back(dy_row.astype(jnp.float32))[0]
        new_sum = tuple(a_sum + g_row for a_sum, g_row in zip(grad_sum, grad_row))
        return new_sum, y_row.astype(jnp.bfloat16)

    grad_total, hidden = lax.scan(scan_step, grad_init, (tokens, grad_y))
    return (hidden,) + tuple(grad_total)
```

```python
import jax
import jax.numpy as jnp
from jax import lax
from jax.experimental import pallas as pl
from jax.experimental.pallas import tpu as pltpu
from jax.sharding import PartitionSpec as P

HEAD_DIM = 64
MASK_ID = 32
PAD_ID = 1
MASK_RATIO = 0.15 * 0.8
LN_EPS = 1e-5
ROPE_BASE = 10000.0
NEG = -1e30
BF16 = jnp.bfloat16
F32 = jnp.float32


def dot_f32(lhs, rhs, lhs_dim, rhs_dim):
    return lax.dot_general(lhs, rhs, (((lhs_dim,), (rhs_dim,)), ((), ())), preferred_element_type=F32)


def norm_fwd(x_val, gain, bias):
    centered = x_val - jnp.mean(x_val, axis=-1, keepdims=True)
    inv_std = lax.rsqrt(jnp.mean(centered * centered, axis=-1, keepdims=True) + LN_EPS)
    x_hat = centered * inv_std
    return x_hat * gain.astype(F32) + bias.astype(F32), x_hat, inv_std


def norm_bwd(d_out, x_hat, inv_std, gain):
    d_hat = d_out * gain.astype(F32)
    d_x = inv_std * (d_hat - jnp.mean(d_hat, axis=-1, keepdims=True)
                     - x_hat * jnp.mean(d_hat * x_hat, axis=-1, keepdims=True))
    return d_x, jnp.sum(d_out * x_hat, axis=0), jnp.sum(d_out, axis=0)


def rope_tables(seq_len):
    inv_freq = 1.0 / (ROPE_BASE ** (jnp.arange(0, HEAD_DIM, 2, dtype=F32) / HEAD_DIM))
    angles = jnp.arange(seq_len, dtype=F32)[:, None] * inv_freq[None, :]
    cos_tab, sin_tab = jnp.cos(angles), jnp.sin(angles)
    return (jnp.concatenate([cos_tab] * 4, axis=1),
            jnp.concatenate([-sin_tab, sin_tab, -sin_tab, sin_tab], axis=1))


def partner_lanes(x_val):
    lane = lax.broadcasted_iota(jnp.int32, x_val.shape, 1)
    half = HEAD_DIM // 2
    return jnp.where(lane % HEAD_DIM < half, pltpu.roll(x_val, 128 - half, 1), pltpu.roll(x_val, half, 1))


def attn_fwd_kernel(q_in, k_in, v_in, cos_ref, sin_ref, pad_ref, q_out, k_out, v_out, ctx_out):
    cos_tab, sin_tab = cos_ref[...], sin_ref[...]
    q_val = q_in[0] * HEAD_DIM ** -0.5
    q_val = (q_val * cos_tab + partner_lanes(q_val) * sin_tab).astype(BF16)
    k_val = k_in[0]
    k_val = (k_val * cos_tab + partner_lanes(k_val) * sin_tab).astype(BF16)
    v_val = v_in[0].astype(BF16)
    q_out[0], k_out[0], v_out[0] = q_val, k_val, v_val
    low = lax.broadcasted_iota(jnp.int32, q_val.shape, 1) < HEAD_DIM
    pad = pad_ref[0, :1, :] > 0.0
    parts = []
    for head in range(2):
        q_head = jnp.where(low if head == 0 else jnp.logical_not(low), q_val, jnp.zeros_like(q_val))
        scores = jnp.where(pad, NEG, dot_f32(q_head, k_val, 1, 1))
        weight = jnp.exp(scores - jnp.max(scores, axis=1, keepdims=True))
        prob = weight * (1.0 / jnp.sum(weight, axis=1, keepdims=True))
        parts.append(dot_f32(prob.astype(BF16), v_val, 1, 0))
    ctx_out[0] = jnp.where(low, parts[0], parts[1]).astype(BF16)


def attn_bwd_kernel(q_in, k_in, v_in, d_in, cos_ref, sin_ref, pad_ref, dq_out, bias_out):
    q_val, k_val, v_val, d_ctx = q_in[0], k_in[0], v_in[0], d_in[0]
    cos_tab, sin_tab = cos_ref[...], sin_ref[...]
    low = lax.broadcasted_iota(jnp.int32, q_val.shape, 1) < HEAD_DIM
    pad = pad_ref[0, :, :1] > 0.0
    zero = jnp.zeros_like(k_val)
    dq_parts, dk_parts, dv_parts = [], [], []
    for head in range(2):
        mine = low if head == 0 else jnp.logical_not(low)
        scores = jnp.where(pad, NEG, dot_f32(jnp.where(mine, k_val, zero), q_val, 1, 1))
        weight = jnp.exp(scores - jnp.max(scores, axis=0, keepdims=True))
        prob = weight * (1.0 / jnp.sum(weight, axis=0, keepdims=True))
        d_prob = dot_f32(jnp.where(mine, v_val, zero), d_ctx, 1, 1)
        delta = jnp.sum(prob * d_prob, axis=0, keepdims=True)
        d_scores = (prob * (d_prob - delta)).astype(BF16)
        dv_parts.append(dot_f32(prob.astype(BF16), d_ctx, 1, 0))
        dk_parts.append(dot_f32(d_scores, q_val, 1, 0))
        dq_parts.append(dot_f32(d_scores, k_val, 0, 0))
    d_q = jnp.where(low, dq_parts[0], dq_parts[1])
    d_k = jnp.where(low, dk_parts[0], dk_parts[1])
    d_v = jnp.where(low, dv_parts[0], dv_parts[1])
    d_q = (d_q * cos_tab - partner_lanes(d_q) * sin_tab) * HEAD_DIM ** -0.5
    d_k = d_k * cos_tab - partner_lanes(d_k) * sin_tab
    pair = pl.program_id(1)
    model_dim = dq_out.shape[2] // 3
    for i, grad in enumerate((d_q, d_k, d_v)):
        lanes = pl.ds(pl.multiple_of(pair * 128 + i * model_dim, 128), 128)
        dq_out[0, :, lanes] = grad.astype(BF16)
        bias_out[0, :, lanes] = jnp.sum(grad.reshape(-1, 8, 128), axis=0)


def attention_fwd(qkv_proj, cos_tab, sin_tab, pad_row):
    rows, seq, width = qkv_proj.shape
    dim = width // 3
    pairs = dim // 128
    blk = lambda shift: pl.BlockSpec((1, seq, 128), lambda b, p: (b, 0, p + shift))
    tab = pl.BlockSpec((seq, 128), lambda b, p: (0, 0))
    out = jax.ShapeDtypeStruct((rows, seq, dim), BF16)
    return pl.pallas_call(
        attn_fwd_kernel, grid=(rows, pairs),
        in_specs=[blk(0), blk(pairs), blk(2 * pairs), tab, tab,
                  pl.BlockSpec((1, 8, seq), lambda b, p: (b, 0, 0))],
        out_specs=[blk(0)] * 4, out_shape=[out] * 4,
        cost_estimate=pl.CostEstimate(flops=int(3e10), bytes_accessed=rows * seq * dim * 20,
                                      transcendentals=rows * seq * seq * 2 * pairs),
        name='attn_fwd',
    )(qkv_proj, qkv_proj, qkv_proj, cos_tab, sin_tab, pad_row)


def attention_bwd(q_val, k_val, v_val, d_ctx, cos_tab, sin_tab, pad_col):
    rows, seq, dim = q_val.shape
    pairs = dim // 128
    blk = pl.BlockSpec((1, seq, 128), lambda b, p: (b, 0, p))
    tab = pl.BlockSpec((seq, 128), lambda b, p: (0, 0))
    return pl.pallas_call(
        attn_bwd_kernel, grid=(rows, pairs),
        in_specs=[blk] * 4 + [tab, tab, pl.BlockSpec((1, seq, 128), lambda b, p: (b, 0, 0))],
        out_specs=[pl.BlockSpec((1, seq, 3 * dim), lambda b, p: (b, 0, 0)),
                   pl.BlockSpec((1, 8, 3 * dim), lambda b, p: (b, 0, 0))],
        out_shape=[jax.ShapeDtypeStruct((rows, seq, 3 * dim), BF16),
                   jax.ShapeDtypeStruct((rows, 8, 3 * dim), F32)],
        cost_estimate=pl.CostEstimate(flops=int(6e10), bytes_accessed=rows * seq * dim * 14,
                                      transcendentals=rows * seq * seq * 2 * pairs),
        name='attn_bwd',
    )(q_val, k_val, v_val, d_ctx, cos_tab, sin_tab, pad_col)


def fc1_kernel(x_ref, w_ref, bias_ref, act_ref, slope_ref):
    pre = jnp.dot(x_ref[...], w_ref[...], preferred_element_type=F32) + bias_ref[:1, :]
    cdf = 0.5 * (1.0 + lax.erf(pre * 0.5 ** 0.5))
    act_ref[...] = (pre * cdf).astype(BF16)
    slope_ref[...] = cdf + pre * (jnp.exp(-0.5 * pre * pre) * (0.5 / jnp.pi) ** 0.5)


def fc1_gelu(x_val, w_val, bias, tile_m=512, tile_n=512):
    rows, dim = x_val.shape
    width = w_val.shape[1]
    out = pl.BlockSpec((tile_m, tile_n), lambda j, i: (i, j))
    return pl.pallas_call(
        fc1_kernel, grid=(width // tile_n, rows // tile_m),
        in_specs=[pl.BlockSpec((tile_m, dim), lambda j, i: (i, 0)), pl.BlockSpec((dim, tile_n), lambda j, i: (0, j)),
                  pl.BlockSpec((8, tile_n), lambda j, i: (0, j))],
        out_specs=[out, out],
        out_shape=[jax.ShapeDtypeStruct((rows, width), BF16), jax.ShapeDtypeStruct((rows, width), F32)],
        cost_estimate=pl.CostEstimate(flops=2 * rows * dim * width, bytes_accessed=rows * width * 6,
                                      transcendentals=rows * width * 2),
        name='fc1_gelu',
    )(x_val, w_val, bias)


def swap(x_val, axis, size, mask):
    return lax.ppermute(x_val, axis, [(i, i ^ mask) for i in range(size)])


def part(x_val, index, count, dim=0):
    size = x_val.shape[dim] // count
    return lax.dynamic_slice_in_dim(x_val, index * size, size, dim)


class Place:
    def __init__(self):
        fsdp, dp = lax.axis_index('fsdp'), lax.axis_index('dp')
        self.core, self.x = fsdp % 2, fsdp // 2
        self.y, self.z = dp % 2, dp // 2
        self.z0, self.z1 = self.z % 2, self.z // 2


def sum_over_dp(place, kept, arrived):
    total, got = kept, arrived
    for bit, mask in ((place.y, 1), (place.z0, 2), (place.z1, 4)):
        total = total + got
        away = part(total, 1 - bit, 2)
        total = part(total, bit, 2)
        got = swap(away, 'dp', 8, mask)
    total = total + got
    pieces = [total] + [swap(total, 'dp', 8, 2 * step) for step in (1, 2, 3)]
    half = jnp.concatenate([lax.select_n(place.z ^ z_of, *pieces) for z_of in (0, 2, 1, 3)], axis=0)
    other = swap(half, 'dp', 8, 1)
    low = place.y == 0
    return jnp.concatenate([jnp.where(low, half, other), jnp.where(low, other, half)], axis=0)


def quarter_cols(x_val, x_index, core_index, count=1, chunk=0):
    return part(x_val, (2 * x_index + core_index) * count + chunk, 4 * count, 1)


def send_half(place, lhs, rhs, count=1, chunk=0):
    cols = jnp.concatenate([quarter_cols(lhs, i, 1 - place.core, count, chunk) for i in range(2)], axis=1)
    return swap(dot_f32(cols, rhs, 0, 0), 'fsdp', 4, 1)


def own_half(place, got, lhs, rhs, count=1, chunk=0):
    away = dot_f32(quarter_cols(lhs, 1 - place.x, place.core, count, chunk), rhs, 0, 0) + part(got, 1 - place.x, 2)
    arrived = swap(away, 'fsdp', 4, 2)
    kept = dot_f32(quarter_cols(lhs, place.x, place.core, count, chunk), rhs, 0, 0) + part(got, place.x, 2)
    return kept, arrived


def small_sum(place, grads):
    wide = grads.reshape(2, 2, -1, 128)
    mine = lax.dynamic_index_in_dim(wide, place.core, 1, False)
    mine = mine + swap(lax.dynamic_index_in_dim(wide, 1 - place.core, 1, False), 'fsdp', 4, 1)
    own = lax.dynamic_index_in_dim(mine, place.x, 0, False)
    own = own + swap(lax.dynamic_index_in_dim(mine, 1 - place.x, 0, False), 'fsdp', 4, 2)
    for mask in (1, 2, 4):
        own = own + swap(own, 'dp', 8, mask)
    return own.reshape(-1)


def solution(mesh):
    row_spec = P(('dp', 'fsdp'), None)
    act_spec = P(('dp', 'fsdp'), None, None)
    param_specs = (P(None, 'fsdp'),) + (P('fsdp'),) * 12

    def local_step(tokens, grad_y, *shards):
        (embedding, ln1_gain, ln1_bias, w_qkv, b_qkv, w_out, b_out,
         ln2_gain, ln2_bias, w_fc1, b_fc1, w_fc2, b_fc2) = shards
        place = Place()
        batch, seq = tokens.shape
        dim = grad_y.shape[2]
        vocab = embedding.shape[0]
        rows = batch * seq

        small = [embedding, ln1_gain, ln1_bias, b_out, ln2_gain, ln2_bias, b_fc2, b_qkv, b_fc1]
        whole = [lax.all_gather(shard, 'fsdp', axis=shard.ndim - 1, tiled=True) for shard in small]
        embedding, ln1_gain, ln1_bias, b_out, ln2_gain, ln2_bias, b_fc2, b_qkv, b_fc1 = whole
        w_qkv, w_out, w_fc1, w_fc2 = [lax.all_gather(w, 'fsdp', axis=0, tiled=True)
                                      for w in (w_qkv, w_out, w_fc1, w_fc2)]

        one_hot = tokens[:, :, None] == jnp.arange(vocab)[None, None, :]
        is_mask = tokens == MASK_ID
        is_pad = tokens == PAD_ID
        mask_count = jnp.sum(is_mask, axis=1).astype(F32)
        real_count = jnp.sum(jnp.logical_not(is_pad), axis=1).astype(F32)
        factor = (1.0 - MASK_RATIO) / (1.0 - mask_count / real_count)
        keep_scale = jnp.where(is_mask | is_pad, 0.0, factor[:, None]).reshape(rows, 1)
        one_hot = one_hot.reshape(rows, vocab)
        looked_up = dot_f32(one_hot.astype(BF16), embedding, 1, 0)
        x_res = (looked_up * keep_scale).astype(BF16).astype(F32)
        norm_one, hat_one, inv_one = norm_fwd(x_res, ln1_gain, ln1_bias)
        h_one = norm_one.astype(BF16)
        qkv_proj = dot_f32(h_one, w_qkv, 1, 0) + b_qkv.astype(F32)
        cos_tab, sin_tab = rope_tables(seq)
        pad_f32 = is_pad.astype(F32)
        queries, key_rows, values, context = attention_fwd(
            qkv_proj.reshape(batch, seq, 3 * dim), cos_tab, sin_tab, jnp.broadcast_to(pad_f32[:, None, :], (batch, 8, seq)))
        context = context.reshape(rows, dim)
        x_mid = x_res + dot_f32(context, w_out, 1, 0) + b_out.astype(F32)
        norm_two, hat_two, inv_two = norm_fwd(x_mid, ln2_gain, ln2_bias)
        h_two = norm_two.astype(BF16)
        act_b16, slope = fc1_gelu(h_two, w_fc1, jnp.broadcast_to(b_fc1.astype(F32)[None, :], (8, b_fc1.size)))

        grad_y = grad_y.reshape(rows, dim)
        grad_res = grad_y.astype(F32)
        got_fc2 = [send_half(place, act_b16, grad_y, 2, j) for j in range(2)]
        d_pre = dot_f32(grad_y, w_fc2, 1, 1) * slope
        g_b_fc1 = jnp.sum(d_pre, axis=0)
        d_pre = d_pre.astype(BF16)
        sums_fc2 = [own_half(place, got_fc2[j], act_b16, grad_y, 2, j) for j in range(2)]
        pre_cols = [d_pre[:, :2 * dim], d_pre[:, 2 * dim:]]
        got_fc1 = [send_half(place, h_two, pre_cols[j]) for j in range(2)]
        d_two, g_ln2_gain, g_ln2_bias = norm_bwd(dot_f32(d_pre, w_fc1, 1, 1), hat_two, inv_two, ln2_gain)
        sums_fc1 = [own_half(place, got_fc1[j], h_two, pre_cols[j]) for j in range(2)]
        d_mid = grad_res + d_two
        g_b_out = jnp.sum(d_mid, axis=0)
        g_b_fc2 = jnp.sum(grad_res, axis=0)
        d_mid_b16 = d_mid.astype(BF16)
        d_ctx = dot_f32(d_mid_b16, w_out, 1, 1).astype(BF16)
        got_out = send_half(place, context, d_mid_b16)
        d_qkv, g_b_qkv = attention_bwd(queries, key_rows, values, d_ctx.reshape(batch, seq, dim),
                                       cos_tab, sin_tab, jnp.broadcast_to(pad_f32[:, :, None], (batch, seq, 128)))
        sums_out = own_half(place, got_out, context, d_mid_b16)
        d_qkv = d_qkv.reshape(rows, 3 * dim)
        g_b_qkv = jnp.sum(g_b_qkv, axis=(0, 1))
        half_qkv = 3 * dim // 2
        qkv_cols = [d_qkv[:, :half_qkv], d_qkv[:, half_qkv:]]
        got_qkv = [send_half(place, h_one, qkv_cols[j]) for j in range(2)]
        d_one, g_ln1_gain, g_ln1_bias = norm_bwd(dot_f32(d_qkv, w_qkv, 1, 1), hat_one, inv_one, ln1_gain)
        sums_qkv = [own_half(place, got_qkv[j], h_one, qkv_cols[j]) for j in range(2)]
        d_in = d_mid + d_one
        g_embedding = dot_f32(one_hot.astype(F32), d_in * keep_scale, 0, 0)
        hidden = (x_mid + dot_f32(act_b16, w_fc2, 1, 0) + b_fc2.astype(F32)).astype(BF16)

        g_w_fc2 = jnp.concatenate([sum_over_dp(place, *sums_fc2[j]) for j in range(2)], axis=0)
        g_w_fc1 = jnp.concatenate([sum_over_dp(place, *sums_fc1[j]) for j in range(2)], axis=1)
        g_w_out = sum_over_dp(place, *sums_out)
        g_w_qkv = jnp.concatenate([sum_over_dp(place, *sums_qkv[j]) for j in range(2)], axis=1)

        small_grads = [g_embedding.reshape(vocab, 4, -1).transpose(1, 0, 2).reshape(4, -1)]
        small_grads += [g.reshape(4, -1) for g in (g_ln1_gain, g_ln1_bias, g_b_out, g_ln2_gain, g_ln2_bias,
                                                   g_b_fc2, g_b_qkv, g_b_fc1)]
        summed = small_sum(place, jnp.concatenate(small_grads, axis=1))
        outs, at = [], 0
        for i, grad in enumerate(small_grads):
            piece = summed[at:at + grad.shape[1]]
            at += grad.shape[1]
            outs.append(piece.reshape(vocab, -1) if i == 0 else piece)
        (g_embedding, g_ln1_gain, g_ln1_bias, g_b_out, g_ln2_gain, g_ln2_bias, g_b_fc2, g_b_qkv, g_b_fc1) = outs
        return (hidden.reshape(batch, seq, dim), g_embedding, g_ln1_gain, g_ln1_bias, g_w_qkv, g_b_qkv, g_w_out,
                g_b_out, g_ln2_gain, g_ln2_bias, g_w_fc1, g_b_fc1, g_w_fc2, g_b_fc2)

    return jax.shard_map(local_step, mesh=mesh, in_specs=(row_spec, act_spec) + param_specs,
                         out_specs=(act_spec,) + param_specs, check_vma=False)
```

```python
import jax
import jax.numpy as jnp
from jax import lax
from jax.experimental import pallas as pl
from jax.experimental.pallas import tpu as pltpu
from jax.sharding import PartitionSpec as P

HEAD_DIM = 64
MASK_ID = 32
PAD_ID = 1
MASK_RATIO = 0.15 * 0.8
LN_EPS = 1e-5
ROPE_BASE = 10000.0
NEG = -1e30
BF16 = jnp.bfloat16
F32 = jnp.float32


def dot_f32(lhs, rhs, lhs_dim, rhs_dim):
    return lax.dot_general(lhs, rhs, (((lhs_dim,), (rhs_dim,)), ((), ())), preferred_element_type=F32)


def norm_fwd(x_val, gain, bias):
    centered = x_val - jnp.mean(x_val, axis=-1, keepdims=True)
    inv_std = lax.rsqrt(jnp.mean(centered * centered, axis=-1, keepdims=True) + LN_EPS)
    x_hat = centered * inv_std
    return x_hat * gain.astype(F32) + bias.astype(F32), x_hat, inv_std


def norm_bwd(d_out, x_hat, inv_std, gain):
    d_hat = d_out * gain.astype(F32)
    d_x = inv_std * (d_hat - jnp.mean(d_hat, axis=-1, keepdims=True)
                     - x_hat * jnp.mean(d_hat * x_hat, axis=-1, keepdims=True))
    return d_x, jnp.sum(d_out * x_hat, axis=0), jnp.sum(d_out, axis=0)


def rope_tables(seq_len):
    inv_freq = 1.0 / (ROPE_BASE ** (jnp.arange(0, HEAD_DIM, 2, dtype=F32) / HEAD_DIM))
    angles = jnp.arange(seq_len, dtype=F32)[:, None] * inv_freq[None, :]
    cos_tab, sin_tab = jnp.cos(angles), jnp.sin(angles)
    return (jnp.concatenate([cos_tab] * 4, axis=1),
            jnp.concatenate([-sin_tab, sin_tab, -sin_tab, sin_tab], axis=1))


def partner_lanes(x_val):
    lane = lax.broadcasted_iota(jnp.int32, x_val.shape, 1)
    half = HEAD_DIM // 2
    return jnp.where(lane % HEAD_DIM < half, pltpu.roll(x_val, 128 - half, 1), pltpu.roll(x_val, half, 1))


def attn_fwd_kernel(q_in, k_in, v_in, cos_ref, sin_ref, pad_ref, q_out, k_out, v_out, ctx_out):
    cos_tab, sin_tab = cos_ref[...], sin_ref[...]
    q_val = q_in[0] * HEAD_DIM ** -0.5
    q_val = (q_val * cos_tab + partner_lanes(q_val) * sin_tab).astype(BF16)
    k_val = k_in[0]
    k_val = (k_val * cos_tab + partner_lanes(k_val) * sin_tab).astype(BF16)
    v_val = v_in[0].astype(BF16)
    q_out[0], k_out[0], v_out[0] = q_val, k_val, v_val
    low = lax.broadcasted_iota(jnp.int32, q_val.shape, 1) < HEAD_DIM
    pad = pad_ref[0, :1, :] > 0.0
    parts = []
    for head in range(2):
        q_head = jnp.where(low if head == 0 else jnp.logical_not(low), q_val, jnp.zeros_like(q_val))
        scores = jnp.where(pad, NEG, dot_f32(q_head, k_val, 1, 1))
        weight = jnp.exp(scores - jnp.max(scores, axis=1, keepdims=True))
        prob = weight * (1.0 / jnp.sum(weight, axis=1, keepdims=True))
        parts.append(dot_f32(prob.astype(BF16), v_val, 1, 0))
    ctx_out[0] = jnp.where(low, parts[0], parts[1]).astype(BF16)


def attn_bwd_kernel(q_in, k_in, v_in, d_in, cos_ref, sin_ref, pad_ref, dq_out, bias_out):
    q_val, k_val, v_val, d_ctx = q_in[0], k_in[0], v_in[0], d_in[0]
    cos_tab, sin_tab = cos_ref[...], sin_ref[...]
    low = lax.broadcasted_iota(jnp.int32, q_val.shape, 1) < HEAD_DIM
    pad = pad_ref[0, :, :1] > 0.0
    zero = jnp.zeros_like(k_val)
    dq_parts, dk_parts, dv_parts = [], [], []
    for head in range(2):
        mine = low if head == 0 else jnp.logical_not(low)
        scores = jnp.where(pad, NEG, dot_f32(jnp.where(mine, k_val, zero), q_val, 1, 1))
        weight = jnp.exp(scores - jnp.max(scores, axis=0, keepdims=True))
        prob = weight * (1.0 / jnp.sum(weight, axis=0, keepdims=True))
        d_prob = dot_f32(jnp.where(mine, v_val, zero), d_ctx, 1, 1)
        delta = jnp.sum(prob * d_prob, axis=0, keepdims=True)
        d_scores = (prob * (d_prob - delta)).astype(BF16)
        dv_parts.append(dot_f32(prob.astype(BF16), d_ctx, 1, 0))
        dk_parts.append(dot_f32(d_scores, q_val, 1, 0))
        dq_parts.append(dot_f32(d_scores, k_val, 0, 0))
    d_q = jnp.where(low, dq_parts[0], dq_parts[1])
    d_k = jnp.where(low, dk_parts[0], dk_parts[1])
    d_v = jnp.where(low, dv_parts[0], dv_parts[1])
    d_q = (d_q * cos_tab - partner_lanes(d_q) * sin_tab) * HEAD_DIM ** -0.5
    d_k = d_k * cos_tab - partner_lanes(d_k) * sin_tab
    pair = pl.program_id(0)
    model_dim = dq_out.shape[2] // 3
    for i, grad in enumerate((d_q, d_k, d_v)):
        lanes = pl.ds(pl.multiple_of(pair * 128 + i * model_dim, 128), 128)
        dq_out[0, :, lanes] = grad.astype(BF16)
        bias_out[0, :, lanes] = jnp.sum(grad.reshape(-1, 8, 128), axis=0)


def attention_fwd(qkv_proj, cos_tab, sin_tab, pad_row):
    rows, seq, width = qkv_proj.shape
    dim = width // 3
    pairs = dim // 128
    blk = lambda shift: pl.BlockSpec((1, seq, 128), lambda b, p: (b, 0, p + shift))
    tab = pl.BlockSpec((seq, 128), lambda b, p: (0, 0))
    out = jax.ShapeDtypeStruct((rows, seq, dim), BF16)
    return pl.pallas_call(
        attn_fwd_kernel, grid=(rows, pairs),
        in_specs=[blk(0), blk(pairs), blk(2 * pairs), tab, tab,
                  pl.BlockSpec((1, 8, seq), lambda b, p: (b, 0, 0))],
        out_specs=[blk(0)] * 4, out_shape=[out] * 4,
        cost_estimate=pl.CostEstimate(flops=int(3e10), bytes_accessed=rows * seq * dim * 20,
                                      transcendentals=rows * seq * seq * 2 * pairs),
        name='attn_fwd',
    )(qkv_proj, qkv_proj, qkv_proj, cos_tab, sin_tab, pad_row)


def attention_bwd(row, d_qkv, d_bias, q_val, k_val, v_val, d_ctx, cos_tab, sin_tab, pad_col):
    rows, seq, dim = q_val.shape
    pairs = dim // 128
    blk = pl.BlockSpec((1, seq, 128), lambda p: (row, 0, p))
    tab = pl.BlockSpec((seq, 128), lambda p: (0, 0))
    operands = [q_val, k_val, v_val, d_ctx, cos_tab, sin_tab, pad_col]
    in_specs = [blk] * 4 + [tab, tab, pl.BlockSpec((1, seq, 128), lambda p: (row, 0, 0))]
    kernel, aliases = attn_bwd_kernel, {}
    if d_qkv is not None:
        def kernel(*refs):
            attn_bwd_kernel(*refs[:7], *refs[9:])

        operands += [d_qkv, d_bias]
        in_specs += [pl.BlockSpec(memory_space=pl.ANY)] * 2
        aliases = {7: 0, 8: 1}
    return pl.pallas_call(
        kernel, grid=(pairs,), in_specs=in_specs,
        out_specs=[pl.BlockSpec((1, seq, 3 * dim), lambda p: (row, 0, 0)),
                   pl.BlockSpec((1, 8, 3 * dim), lambda p: (row, 0, 0))],
        out_shape=[jax.ShapeDtypeStruct((rows, seq, 3 * dim), BF16),
                   jax.ShapeDtypeStruct((rows, 8, 3 * dim), F32)],
        input_output_aliases=aliases,
        cost_estimate=pl.CostEstimate(flops=int(2e10), bytes_accessed=seq * dim * 14,
                                      transcendentals=seq * seq * 2 * pairs),
        name='attn_bwd',
    )(*operands)


def fc1_kernel(x_ref, w_ref, bias_ref, act_ref, slope_ref):
    pre = jnp.dot(x_ref[...], w_ref[...], preferred_element_type=F32) + bias_ref[:1, :]
    cdf = 0.5 * (1.0 + lax.erf(pre * 0.5 ** 0.5))
    act_ref[...] = (pre * cdf).astype(BF16)
    slope_ref[...] = cdf + pre * (jnp.exp(-0.5 * pre * pre) * (0.5 / jnp.pi) ** 0.5)


def fc1_gelu(x_val, w_val, bias, tile_m=512, tile_n=512):
    rows, dim = x_val.shape
    width = w_val.shape[1]
    out = pl.BlockSpec((tile_m, tile_n), lambda j, i: (i, j))
    return pl.pallas_call(
        fc1_kernel, grid=(width // tile_n, rows // tile_m),
        in_specs=[pl.BlockSpec((tile_m, dim), lambda j, i: (i, 0)), pl.BlockSpec((dim, tile_n), lambda j, i: (0, j)),
                  pl.BlockSpec((8, tile_n), lambda j, i: (0, j))],
        out_specs=[out, out],
        out_shape=[jax.ShapeDtypeStruct((rows, width), BF16), jax.ShapeDtypeStruct((rows, width), F32)],
        cost_estimate=pl.CostEstimate(flops=2 * rows * dim * width, bytes_accessed=rows * width * 6,
                                      transcendentals=rows * width * 2),
        name='fc1_gelu',
    )(x_val, w_val, bias)


def swap(x_val, axis, size, mask):
    return lax.ppermute(x_val, axis, [(i, i ^ mask) for i in range(size)])


def part(x_val, index, count, dim=0):
    size = x_val.shape[dim] // count
    return lax.dynamic_slice_in_dim(x_val, index * size, size, dim)


class Place:
    def __init__(self):
        fsdp, dp = lax.axis_index('fsdp'), lax.axis_index('dp')
        self.core, self.x = fsdp % 2, fsdp // 2
        self.y, self.z = dp % 2, dp // 2
        self.z0, self.z1 = self.z % 2, self.z // 2


def sum_over_dp(place, kept, arrived):
    total, got = kept, arrived
    for bit, mask in ((place.y, 1), (place.z0, 2), (place.z1, 4)):
        total = total + got
        away = part(total, 1 - bit, 2)
        total = part(total, bit, 2)
        got = swap(away, 'dp', 8, mask)
    total = total + got
    pieces = [total] + [swap(total, 'dp', 8, 2 * step) for step in (1, 2, 3)]
    half = jnp.concatenate([lax.select_n(place.z ^ z_of, *pieces) for z_of in (0, 2, 1, 3)], axis=0)
    other = swap(half, 'dp', 8, 1)
    low = place.y == 0
    return jnp.concatenate([jnp.where(low, half, other), jnp.where(low, other, half)], axis=0)


def quarter_cols(x_val, x_index, core_index, count=1, chunk=0):
    return part(x_val, (2 * x_index + core_index) * count + chunk, 4 * count, 1)


def send_half(place, lhs, rhs, count=1, chunk=0):
    cols = jnp.concatenate([quarter_cols(lhs, i, 1 - place.core, count, chunk) for i in range(2)], axis=1)
    return swap(dot_f32(cols, rhs, 0, 0), 'fsdp', 4, 1)


def own_half(place, got, lhs, rhs, count=1, chunk=0):
    away = dot_f32(quarter_cols(lhs, 1 - place.x, place.core, count, chunk), rhs, 0, 0) + part(got, 1 - place.x, 2)
    arrived = swap(away, 'fsdp', 4, 2)
    kept = dot_f32(quarter_cols(lhs, place.x, place.core, count, chunk), rhs, 0, 0) + part(got, place.x, 2)
    return kept, arrived


def small_sum(place, grads):
    wide = grads.reshape(2, 2, -1, 128)
    mine = lax.dynamic_index_in_dim(wide, place.core, 1, False)
    mine = mine + swap(lax.dynamic_index_in_dim(wide, 1 - place.core, 1, False), 'fsdp', 4, 1)
    own = lax.dynamic_index_in_dim(mine, place.x, 0, False)
    own = own + swap(lax.dynamic_index_in_dim(mine, 1 - place.x, 0, False), 'fsdp', 4, 2)
    for mask in (1, 2, 4):
        own = own + swap(own, 'dp', 8, mask)
    return own.reshape(-1)


def solution(mesh):
    row_spec = P(('dp', 'fsdp'), None)
    act_spec = P(('dp', 'fsdp'), None, None)
    param_specs = (P(None, 'fsdp'),) + (P('fsdp'),) * 12

    def local_step(tokens, grad_y, *shards):
        (embedding, ln1_gain, ln1_bias, w_qkv, b_qkv, w_out, b_out,
         ln2_gain, ln2_bias, w_fc1, b_fc1, w_fc2, b_fc2) = shards
        place = Place()
        batch, seq = tokens.shape
        dim = grad_y.shape[2]
        vocab = embedding.shape[0]
        rows = batch * seq

        small = [embedding, ln1_gain, ln1_bias, b_out, ln2_gain, ln2_bias, b_fc2, b_qkv, b_fc1]
        whole = [lax.all_gather(shard, 'fsdp', axis=shard.ndim - 1, tiled=True) for shard in small]
        embedding, ln1_gain, ln1_bias, b_out, ln2_gain, ln2_bias, b_fc2, b_qkv, b_fc1 = whole
        w_qkv, w_out, w_fc1, w_fc2 = [lax.all_gather(w, 'fsdp', axis=0, tiled=True)
                                      for w in (w_qkv, w_out, w_fc1, w_fc2)]

        one_hot = tokens[:, :, None] == jnp.arange(vocab)[None, None, :]
        is_mask = tokens == MASK_ID
        is_pad = tokens == PAD_ID
        mask_count = jnp.sum(is_mask, axis=1).astype(F32)
        real_count = jnp.sum(jnp.logical_not(is_pad), axis=1).astype(F32)
        factor = (1.0 - MASK_RATIO) / (1.0 - mask_count / real_count)
        keep_scale = jnp.where(is_mask | is_pad, 0.0, factor[:, None]).reshape(rows, 1)
        one_hot = one_hot.reshape(rows, vocab)
        looked_up = dot_f32(one_hot.astype(BF16), embedding, 1, 0)
        x_res = (looked_up * keep_scale).astype(BF16).astype(F32)
        norm_one, hat_one, inv_one = norm_fwd(x_res, ln1_gain, ln1_bias)
        h_one = norm_one.astype(BF16)
        qkv_proj = dot_f32(h_one, w_qkv, 1, 0) + b_qkv.astype(F32)
        cos_tab, sin_tab = rope_tables(seq)
        pad_f32 = is_pad.astype(F32)
        queries, key_rows, values, context = attention_fwd(
            qkv_proj.reshape(batch, seq, 3 * dim), cos_tab, sin_tab, jnp.broadcast_to(pad_f32[:, None, :], (batch, 8, seq)))
        context = context.reshape(rows, dim)
        x_mid = x_res + dot_f32(context, w_out, 1, 0) + b_out.astype(F32)
        norm_two, hat_two, inv_two = norm_fwd(x_mid, ln2_gain, ln2_bias)
        h_two = norm_two.astype(BF16)
        act_b16, slope = fc1_gelu(h_two, w_fc1, jnp.broadcast_to(b_fc1.astype(F32)[None, :], (8, b_fc1.size)))

        grad_y = grad_y.reshape(rows, dim)
        grad_res = grad_y.astype(F32)
        got_fc2 = [send_half(place, act_b16, grad_y, 2, j) for j in range(2)]
        d_pre = dot_f32(grad_y, w_fc2, 1, 1) * slope
        g_b_fc1 = jnp.sum(d_pre, axis=0)
        d_pre = d_pre.astype(BF16)
        sums_fc2 = [own_half(place, got_fc2[j], act_b16, grad_y, 2, j) for j in range(2)]
        pre_cols = [d_pre[:, :2 * dim], d_pre[:, 2 * dim:]]
        got_fc1 = [send_half(place, h_two, pre_cols[j]) for j in range(2)]
        d_two, g_ln2_gain, g_ln2_bias = norm_bwd(dot_f32(d_pre, w_fc1, 1, 1), hat_two, inv_two, ln2_gain)
        sums_fc1 = [own_half(place, got_fc1[j], h_two, pre_cols[j]) for j in range(2)]
        d_mid = grad_res + d_two
        g_b_out = jnp.sum(d_mid, axis=0)
        g_b_fc2 = jnp.sum(grad_res, axis=0)
        d_mid_b16 = d_mid.astype(BF16)
        d_ctx = dot_f32(d_mid_b16, w_out, 1, 1).astype(BF16)
        got_out = send_half(place, context, d_mid_b16)
        d_qkv = g_b_qkv = None
        for b in range(batch):
            d_qkv, g_b_qkv = attention_bwd(
                b, d_qkv, g_b_qkv, queries, key_rows, values, d_ctx.reshape(batch, seq, dim), cos_tab, sin_tab, jnp.broadcast_to(pad_f32[:, :, None], (batch, seq, 128)))
        sums_out = own_half(place, got_out, context, d_mid_b16)
        d_qkv = d_qkv.reshape(rows, 3 * dim)
        g_b_qkv = jnp.sum(g_b_qkv, axis=(0, 1))
        half_qkv = 3 * dim // 2
        qkv_cols = [d_qkv[:, :half_qkv], d_qkv[:, half_qkv:]]
        got_qkv = [send_half(place, h_one, qkv_cols[j]) for j in range(2)]
        d_one, g_ln1_gain, g_ln1_bias = norm_bwd(dot_f32(d_qkv, w_qkv, 1, 1), hat_one, inv_one, ln1_gain)
        sums_qkv = [own_half(place, got_qkv[j], h_one, qkv_cols[j]) for j in range(2)]
        d_in = d_mid + d_one
        g_embedding = dot_f32(one_hot.astype(F32), d_in * keep_scale, 0, 0)
        hidden = (x_mid + dot_f32(act_b16, w_fc2, 1, 0) + b_fc2.astype(F32)).astype(BF16)

        g_w_fc2 = jnp.concatenate([sum_over_dp(place, *sums_fc2[j]) for j in range(2)], axis=0)
        g_w_fc1 = jnp.concatenate([sum_over_dp(place, *sums_fc1[j]) for j in range(2)], axis=1)
        g_w_out = sum_over_dp(place, *sums_out)
        g_w_qkv = jnp.concatenate([sum_over_dp(place, *sums_qkv[j]) for j in range(2)], axis=1)

        small_grads = [g_embedding.reshape(vocab, 4, -1).transpose(1, 0, 2).reshape(4, -1)]
        small_grads += [g.reshape(4, -1) for g in (g_ln1_gain, g_ln1_bias, g_b_out, g_ln2_gain, g_ln2_bias,
                                                   g_b_fc2, g_b_qkv, g_b_fc1)]
        summed = small_sum(place, jnp.concatenate(small_grads, axis=1))
        outs, at = [], 0
        for i, grad in enumerate(small_grads):
            piece = summed[at:at + grad.shape[1]]
            at += grad.shape[1]
            outs.append(piece.reshape(vocab, -1) if i == 0 else piece)
        (g_embedding, g_ln1_gain, g_ln1_bias, g_b_out, g_ln2_gain, g_ln2_bias, g_b_fc2, g_b_qkv, g_b_fc1) = outs
        return (hidden.reshape(batch, seq, dim), g_embedding, g_ln1_gain, g_ln1_bias, g_w_qkv, g_b_qkv, g_w_out,
                g_b_out, g_ln2_gain, g_ln2_bias, g_w_fc1, g_b_fc1, g_w_fc2, g_b_fc2)

    return jax.shard_map(local_step, mesh=mesh, in_specs=(row_spec, act_spec) + param_specs,
                         out_specs=(act_spec,) + param_specs, check_vma=False)
```
